256 devices in a mesh: section: 8 (over z_lo, y), dp: 32 (over x, z_hi, core).
Axes of the slice: x: 4, y: 4, z: 8 (z_hi: 4, z_lo: 2; z = z_hi * 2 + z_lo), core: 2. Of those that a mesh axis runs over, the one named last changes fastest.
Arguments:
- inputs: bfloat16 [256, 128, 1536], P('dp'), parts along dimension 0, may hold values from -6 to 6
- w_query: bfloat16 [8, 1536, 768], P('section'), may hold values from -0.15625 to 0.15625
- w_key: bfloat16 [8, 1536, 768], P('section'), may hold values from -0.15625 to 0.15625
- w_value: bfloat16 [8, 1536, 768], P('section'), may hold values from -0.15625 to 0.15625
- w_out: bfloat16 [8, 768, 1536], P('section'), may hold values from -0.21875 to 0.21875
- mixing: float32 [8], P('section'), may hold values from 0.2 to 0.8
Outputs:
- outputs: bfloat16 [256, 128, 1536], P(('dp', 'section')), parts along dimension 0
The draws below stay inside these ranges and needn't reach their ends.
There are 32 independent parts, one for each index of `dp`. The reference program is written for one: setup_inputs(seed, part) draws one part's arguments, and reference() takes and returns one part's arrays. A program takes and returns all parts, laid end to end along the dimension named above; an argument that names none is the same for every part. Nothing has to cross between parts.
All inputs are finite; a program needn't handle non-finite values.
Results may differ from the reference program's by a relative error of at most 0.023.
Values may be sent and summed in bfloat16 or wider, within the bound.
A program may use at most 128 MiB of HBM per device.

```python
import jax
import jax.numpy as jnp
from jax import lax

D = 1536
HEADS = 6
HEAD_DIM = 128
SEQ = 128
HD = 768
MICRO = 8
LAYERS = 8


def level_of(stream_key, dims, split, low, top_value):
    def one(position, shards_of):
        draws = jax.random.uniform(jax.random.fold_in(jax.random.fold_in(stream_key, 6), position), (shards_of,), jnp.float32, low / len(split), top_value / len(split))
        return jnp.repeat(jnp.exp(draws), dims[position] // shards_of).reshape((-1,) + (1,) * (len(dims) - position - 1))

    gain = one(*split[0])
    for cut in split[1:]:
        gain = gain * one(*cut)
    return gain


def scatter_about(key, dims, width, reach, pieces=(), kind=jnp.bfloat16):
    entries = jax.random.normal(key, dims, jnp.float32) * width
    if len(pieces) > 0:
        entries = level_of(key, dims, pieces, -0.22, 0.18) * entries
    return jnp.clip(entries, min=-reach, max=reach).astype(kind)


def setup_inputs(seed: int = 0, part: int = 0) -> dict:
    key_of = jax.random.split(jax.random.key(seed), 7)
    part_keys = jax.random.split(jax.random.fold_in(key_of[6], part), 7)
    inputs = scatter_about(part_keys[0], (MICRO, SEQ, D), 1.0, 6.0)
    w_query = scatter_about(key_of[1], (LAYERS, D, HD), D ** -0.5, 0.15625, ((0, 8),))
    w_key = scatter_about(key_of[2], (LAYERS, D, HD), D ** -0.5, 0.15625, ((0, 8),))
    w_value = scatter_about(key_of[3], (LAYERS, D, HD), D ** -0.5, 0.15625, ((0, 8),))
    w_out = scatter_about(key_of[4], (LAYERS, HD, D), HD ** -0.5, 0.21875, ((0, 8),))
    mixing = jnp.clip(0.2 + 0.6 * jax.random.uniform(key_of[5], (LAYERS,), jnp.float32) ** level_of(key_of[5], (LAYERS,), ((0, 8),), -0.2, 0.2), 0.2, 0.8)
    return dict(inputs=inputs, w_query=w_query, w_key=w_key, w_value=w_value, w_out=w_out, mixing=mixing)


epsilon = 1e-06
score_scale = 0.12

def norm_rows(tensor):
    return tensor * lax.rsqrt(lax.optimization_barrier(jnp.mean(tensor * tensor, axis=-1, keepdims=True)) + epsilon)

def layer_apply(hidden, w_query, w_key, w_value, w_out, mixing, first_values, first_flag):
    row_count = hidden.shape[0]
    hidden_wide = hidden.astype(jnp.float32)
    normed = norm_rows(hidden_wide).astype(jnp.bfloat16)
    queries = jnp.dot(normed, w_query, preferred_element_type=jnp.float32).reshape(row_count, HEADS, HEAD_DIM)
    key_rows = jnp.dot(normed, w_key, preferred_element_type=jnp.float32).reshape(row_count, HEADS, HEAD_DIM)
    queries = norm_rows(queries).astype(jnp.bfloat16)
    key_rows = norm_rows(key_rows).astype(jnp.bfloat16)
    values = jnp.dot(normed, w_value, preferred_element_type=jnp.float32)
    own_values = values.astype(jnp.bfloat16)
    if first_flag:
        used_values = own_values
    else:
        used_values = (mixing * values + (1.0 - mixing) * first_values.astype(jnp.float32)).astype(jnp.bfloat16)
    used_values = used_values.reshape(row_count, HEADS, HEAD_DIM)
    scores = jnp.einsum('qhd,khd->hqk', queries.astype(jnp.float32), key_rows.astype(jnp.float32)) * score_scale
    positions = jnp.arange(row_count, dtype=jnp.int32)
    causal = positions[:, None] >= positions[None, :]
    weights = jnp.where(causal[None, :, :], jnp.exp(scores), 0.0)
    probabilities = (weights / lax.optimization_barrier(jnp.sum(weights, axis=-1, keepdims=True))).astype(jnp.bfloat16)
    attended = jnp.einsum('hqk,khd->qhd', probabilities.astype(jnp.float32), used_values.astype(jnp.float32))
    attended = attended.astype(jnp.bfloat16).reshape(row_count, HEADS * HEAD_DIM)
    result = (hidden_wide + jnp.dot(attended, w_out, preferred_element_type=jnp.float32)).astype(jnp.bfloat16)
    return (result, own_values)

def reference(inputs, w_query, w_key, w_value, w_out, mixing):
    finished = []
    for micro_index in range(inputs.shape[0]):
        hidden = inputs[micro_index]
        first_values = None
        for layer_number in range(w_query.shape[0]):
            hidden, own_values = layer_apply(hidden, w_query[layer_number], w_key[layer_number], w_value[layer_number], w_out[layer_number], mixing[layer_number], first_values, layer_number == 0)
            if layer_number == 0:
                first_values = own_values
        finished.append(hidden)
    return jnp.stack(finished)
```

```python
import functools

import jax
import jax.numpy as jnp
from jax import lax
from jax.experimental import pallas as pl
from jax.experimental.pallas import tpu as pltpu
from jax.sharding import PartitionSpec as P

MESH = pl.DeviceIdType.MESH
HEADS = 6
ROWS = 32
LEAD = {3: 9, 2: 4}

epsilon = 1e-06
score_scale = 0.12


def inverse_norm(tensor):
    return lax.rsqrt(jnp.mean(tensor * tensor, axis=-1, keepdims=True) + epsilon)


def kernel(
    sections,
    x_hbm,
    wq_hbm,
    wk_hbm,
    wv_hbm,
    wo_hbm,
    mix_ref,
    out_hbm,
    wq,
    wk,
    wv,
    wo,
    arrived,
    leaving,
    first,
    key_cache,
    value_cache,
    result,
    weight_sem,
    arrive_sem,
    leave_sem,
    first_sem,
    first_y_sem,
    first_z_sem,
    result_sem,
    out_sem,
):
    me = lax.axis_index("section")
    last = sections - 1
    half = sections // 2
    micro, seq, width = x_hbm.shape
    head_dim = wq.shape[1] // HEADS
    cuts = seq // ROWS
    pieces = micro * cuts
    bf16 = jnp.bfloat16

    weight_copies = [
        pltpu.make_async_copy(source.at[0], target, weight_sem.at[n])
        for n, (source, target) in enumerate(
            ((wq_hbm, wq), (wk_hbm, wk), (wv_hbm, wv), (wo_hbm, wo))
        )
    ]

    def input_copy(index):
        rows = pl.ds(pl.multiple_of(lax.rem(index, cuts) * ROWS, ROWS), ROWS)
        return pltpu.make_async_copy(
            x_hbm.at[index // cuts, rows], arrived.at[index], arrive_sem.at[index]
        )

    def hidden_copy(index):
        return pltpu.make_async_remote_copy(
            src_ref=leaving.at[index],
            dst_ref=arrived.at[index],
            send_sem=leave_sem.at[index],
            recv_sem=arrive_sem.at[index],
            device_id={"section": lax.rem(me + 1, sections)},
            device_id_type=MESH,
        )

    def result_copy(index):
        return pltpu.make_async_remote_copy(
            src_ref=leaving.at[index],
            dst_ref=result.at[lax.rem(index, cuts)],
            send_sem=leave_sem.at[index],
            recv_sem=result_sem.at[lax.rem(index, cuts)],
            device_id={"section": index // cuts},
            device_id_type=MESH,
        )

    def first_along_y(index):
        target = jnp.where(me == 0, half - 1, me - 1)
        return pltpu.make_async_remote_copy(
            src_ref=first.at[index],
            dst_ref=first.at[index],
            send_sem=first_y_sem.at[index],
            recv_sem=first_sem.at[index],
            device_id={"section": target},
            device_id_type=MESH,
        )

    def first_along_z(index):
        return pltpu.make_async_remote_copy(
            src_ref=first.at[index],
            dst_ref=first.at[index],
            send_sem=first_z_sem.at[index],
            recv_sem=first_sem.at[index],
            device_id={"section": lax.rem(me + half, sections)},
            device_id_type=MESH,
        )

    @pl.when(me == 0)
    def _():
        input_copy(0).start()

    for copy in weight_copies:
        copy.start()

    @pl.when(me == 0)
    def _():
        @pl.loop(1, pieces)
        def _(index):
            input_copy(index).start()

    barrier = pltpu.get_barrier_semaphore()
    for step in range(1, sections):
        pl.semaphore_signal(
            barrier,
            inc=1,
            device_id={"section": lax.rem(me + step, sections)},
            device_id_type=MESH,
        )
    key_cache[...] = jnp.zeros_like(key_cache)
    value_cache[...] = jnp.zeros_like(value_cache)
    pl.semaphore_wait(barrier, sections - 1)
    for copy in weight_copies:
        copy.wait()

    passes_on = jnp.logical_and(me >= 2, me < half)
    lead = jnp.where(me == 3, LEAD[3], LEAD[2])

    def pass_on(index):
        first_along_y(index).wait_recv()
        first_along_y(index).start()

    @pl.when(passes_on)
    def _():
        @pl.loop(0, lead)
        def _(index):
            pass_on(index)

    share = jnp.where(me == 0, 1.0, mix_ref[0])

    @pl.loop(0, pieces)
    def _(index):
        cut = lax.rem(index, cuts)
        start = pl.multiple_of(cut * ROWS, ROWS)
        rows = pl.ds(start, ROWS)

        input_copy(index).wait()

        hidden = arrived[index].astype(jnp.float32)
        normed = (hidden * inverse_norm(hidden)).astype(bf16)
        queries = jnp.dot(normed, wq[...], preferred_element_type=jnp.float32)
        keys = jnp.dot(normed, wk[...], preferred_element_type=jnp.float32)
        values = jnp.dot(normed, wv[...], preferred_element_type=jnp.float32)

        @pl.when(me == 0)
        def _():
            first[index] = values.astype(bf16)
            first_along_y(index).start()

        @pl.when(jnp.logical_or(me == 1, me >= half))
        def _():
            first_along_y(index).wait_recv()

        @pl.when(jnp.logical_and(passes_on, index + lead < pieces))
        def _():
            pass_on(index + lead)

        @pl.when(me < half)
        def _():
            first_along_z(index).start()

        used = share * values + (1.0 - share) * first[index].astype(jnp.float32)
        value_cache[rows, :] = used.astype(bf16)

        heads = [slice(n * head_dim, (n + 1) * head_dim) for n in range(HEADS)]
        for head in heads:
            part = keys[:, head]
            key_cache[rows, head] = (part * inverse_norm(part)).astype(bf16)
        query_parts = []
        for head in heads:
            part = queries[:, head]
            query_parts.append((part * inverse_norm(part)).astype(bf16))
        query_at = start + lax.broadcasted_iota(jnp.int32, (ROWS, seq), 0)
        key_at = lax.broadcasted_iota(jnp.int32, (ROWS, seq), 1)
        causal = query_at >= key_at
        probabilities = []
        for head, part in zip(heads, query_parts):
            scores = score_scale * lax.dot_general(
                part,
                key_cache[:, head],
                (((1,), (1,)), ((), ())),
                preferred_element_type=jnp.float32,
            )
            weights = jnp.where(causal, jnp.exp(scores), 0.0)
            total = jnp.sum(weights, axis=-1, keepdims=True)
            probabilities.append((weights * (1.0 / total)).astype(bf16))
        attended = jnp.concatenate(
            [
                jnp.dot(
                    part, value_cache[:, head], preferred_element_type=jnp.float32
                ).astype(bf16)
                for head, part in zip(heads, probabilities)
            ],
            axis=1,
        )
        added = jnp.dot(attended, wo[...], preferred_element_type=jnp.float32)
        following = (hidden + added).astype(bf16)
        leaving[index] = following

        @pl.when(me < last)
        def _():
            hidden_copy(index).start()

        @pl.when(me == last)
        def _():
            @pl.when(index // cuts < last)
            def _():
                result_copy(index).start()

            @pl.when(index // cuts == last)
            def _():
                result[cut] = following

    @pl.when(me < last)
    def _():
        @pl.loop(0, cuts)
        def _(index):
            result_copy(index).wait_recv()

    out_copies = [
        pltpu.make_async_copy(
            result.at[n], out_hbm.at[0, pl.ds(n * ROWS, ROWS)], out_sem.at[n]
        )
        for n in range(cuts)
    ]
    for copy in out_copies:
        copy.start()

    @pl.loop(0, pieces)
    def _(index):
        @pl.when(jnp.logical_or(me < last, index // cuts < last))
        def _():
            hidden_copy(index).wait_send()

        @pl.when(jnp.logical_or(me == 0, passes_on))
        def _():
            first_along_y(index).wait_send()

        @pl.when(me < half)
        def _():
            first_along_z(index).wait_send()

    for copy in out_copies:
        copy.wait()


def body(inputs, w_query, w_key, w_value, w_out, mixing):
    sections = lax.axis_size("section")
    micro, seq, width = inputs.shape
    inner = w_query.shape[2]
    cuts = seq // ROWS
    pieces = micro * cuts
    anywhere = pl.BlockSpec(memory_space=pl.ANY)
    dma = pltpu.SemaphoreType.DMA
    return pl.pallas_call(
        functools.partial(kernel, sections),
        out_shape=jax.ShapeDtypeStruct((micro // sections, seq, width), jnp.bfloat16),
        in_specs=[anywhere] * 5 + [pl.BlockSpec(memory_space=pltpu.SMEM)],
        out_specs=anywhere,
        scratch_shapes=[
            pltpu.VMEM((width, inner), jnp.bfloat16),
            pltpu.VMEM((width, inner), jnp.bfloat16),
            pltpu.VMEM((width, inner), jnp.bfloat16),
            pltpu.VMEM((inner, width), jnp.bfloat16),
            pltpu.VMEM((pieces, ROWS, width), jnp.bfloat16),
            pltpu.VMEM((pieces, ROWS, width), jnp.bfloat16),
            pltpu.VMEM((pieces, ROWS, inner), jnp.bfloat16),
            pltpu.VMEM((seq, inner), jnp.bfloat16),
            pltpu.VMEM((seq, inner), jnp.bfloat16),
            pltpu.VMEM((cuts, ROWS, width), jnp.bfloat16),
            dma((4,)),
            dma((pieces,)),
            dma((pieces,)),
            dma((pieces,)),
            dma((pieces,)),
            dma((pieces,)),
            dma((cuts,)),
            dma((cuts,)),
        ],
        compiler_params=pltpu.CompilerParams(
            collective_id=0, has_side_effects=True, vmem_limit_bytes=60 * 2**20
        ),
    )(inputs, w_query, w_key, w_value, w_out, mixing)


def solution(mesh):
    in_specs = (
        P("dp", None, None),
        P("section", None, None),
        P("section", None, None),
        P("section", None, None),
        P("section", None, None),
        P("section"),
    )
    out_specs = P(("dp", "section"), None, None)
    return jax.shard_map(body, mesh=mesh, in_specs=in_specs, out_specs=out_specs, check_vma=False)
```

```python
import functools

import jax
import jax.numpy as jnp
from jax import lax
from jax.experimental import pallas as pl
from jax.experimental.pallas import tpu as pltpu
from jax.sharding import PartitionSpec as P

MESH = pl.DeviceIdType.MESH
HEADS = 6
ROWS = 32
LEAD = {3: 14, 2: 5}
DIRECT = 2

epsilon = 1e-06
score_scale = 0.12


def inverse_norm(tensor):
    return lax.rsqrt(jnp.mean(tensor * tensor, axis=-1, keepdims=True) + epsilon)


def kernel(
    sections,
    x_hbm,
    wq_hbm,
    wk_hbm,
    wv_hbm,
    wo_hbm,
    mix_ref,
    out_hbm,
    wq,
    wk,
    wv,
    wo,
    arrived,
    leaving,
    first,
    key_cache,
    value_cache,
    result,
    weight_sem,
    arrive_sem,
    leave_sem,
    first_sem,
    first_y_sem,
    first_z_sem,
    first_direct_sem,
    result_sem,
    out_sem,
):
    me = lax.axis_index("section")
    last = sections - 1
    half = sections // 2
    micro, seq, width = x_hbm.shape
    head_dim = wq.shape[1] // HEADS
    cuts = seq // ROWS
    pieces = micro * cuts
    bf16 = jnp.bfloat16

    weight_copies = [
        pltpu.make_async_copy(source.at[0], target, weight_sem.at[n])
        for n, (source, target) in enumerate(
            ((wv_hbm, wv), (wq_hbm, wq), (wk_hbm, wk), (wo_hbm, wo))
        )
    ]

    def input_copy(index):
        rows = pl.ds(pl.multiple_of(lax.rem(index, cuts) * ROWS, ROWS), ROWS)
        return pltpu.make_async_copy(
            x_hbm.at[index // cuts, rows], arrived.at[index], arrive_sem.at[index]
        )

    def hidden_copy(index):
        return pltpu.make_async_remote_copy(
            src_ref=leaving.at[index],
            dst_ref=arrived.at[index],
            send_sem=leave_sem.at[index],
            recv_sem=arrive_sem.at[index],
            device_id={"section": lax.rem(me + 1, sections)},
            device_id_type=MESH,
        )

    def result_copy(index):
        return pltpu.make_async_remote_copy(
            src_ref=leaving.at[index],
            dst_ref=result.at[lax.rem(index, cuts)],
            send_sem=leave_sem.at[index],
            recv_sem=result_sem.at[lax.rem(index, cuts)],
            device_id={"section": index // cuts},
            device_id_type=MESH,
        )

    def first_along_y(index):
        target = jnp.where(me % half == 0, me + half - 1, me - 1)
        return pltpu.make_async_remote_copy(
            src_ref=first.at[index],
            dst_ref=first.at[index],
            send_sem=first_y_sem.at[index],
            recv_sem=first_sem.at[index],
            device_id={"section": target},
            device_id_type=MESH,
        )

    def first_along_z(index):
        return pltpu.make_async_remote_copy(
            src_ref=first.at[index],
            dst_ref=first.at[index],
            send_sem=first_z_sem.at[index],
            recv_sem=first_sem.at[index],
            device_id={"section": lax.rem(me + half, sections)},
            device_id_type=MESH,
        )

    def first_direct(index):
        return pltpu.make_async_remote_copy(
            src_ref=first.at[index],
            dst_ref=first.at[index],
            send_sem=first_direct_sem.at[index],
            recv_sem=first_sem.at[index],
            device_id={"section": 1},
            device_id_type=MESH,
        )

    @pl.when(me == 0)
    def _():
        for n in range(cuts):
            input_copy(n).start()

    for copy in weight_copies:
        copy.start()

    @pl.when(me == 0)
    def _():
        @pl.loop(cuts, pieces)
        def _(index):
            input_copy(index).start()

    barrier = pltpu.get_barrier_semaphore()
    for step in range(1, sections):
        pl.semaphore_signal(
            barrier,
            inc=1,
            device_id={"section": lax.rem(me + step, sections)},
            device_id_type=MESH,
        )
    key_cache[...] = jnp.zeros_like(key_cache)
    value_cache[...] = jnp.zeros_like(value_cache)
    pl.semaphore_wait(barrier, sections - 1)

    f32 = jnp.float32
    passes_on = jnp.logical_and(me >= 2, me < half)
    lead = jnp.where(me == half - 1, LEAD[3], LEAD[2])
    share = mix_ref[0]

    def pass_on(index):
        first_along_y(index).wait_recv()

        @pl.when(jnp.logical_or(me == half - 1, index >= DIRECT))
        def _():
            first_along_y(index).start()

        @pl.when(me == 2)
        def _():
            first_along_z(index).start()

    def make_first(sequence):
        base = sequence * cuts
        for n in range(cuts):
            input_copy(base + n).wait()
        packed = jnp.concatenate([arrived[base + n] for n in range(cuts)], axis=0)
        scale = inverse_norm(packed.astype(f32))
        values = scale * jnp.dot(packed, wv[...], preferred_element_type=f32)
        for n in range(cuts):
            first[base + n] = values[n * ROWS : (n + 1) * ROWS].astype(bf16)
        for n in range(cuts):
            first_along_y(base + n).start()
            first_along_z(base + n).start()

    def layer(index, origin):
        cut = lax.rem(index, cuts)
        start = pl.multiple_of(cut * ROWS, ROWS)
        rows = pl.ds(start, ROWS)
        packed = arrived[index]
        hidden = packed.astype(f32)
        scale = inverse_norm(hidden)
        query_at = start + lax.broadcasted_iota(jnp.int32, (2 * ROWS, seq), 0) % ROWS
        key_at = lax.broadcasted_iota(jnp.int32, (2 * ROWS, seq), 1)
        causal = query_at >= key_at
        blank = jnp.zeros((ROWS, head_dim), bf16)
        pair = 2 * head_dim
        depth = width // 2

        def queries_keys(columns):
            return [
                scale * jnp.dot(packed, w[:, columns], preferred_element_type=f32)
                for w in (wq, wk)
            ]

        def used_values(columns):
            if origin:
                value_cache[rows, columns] = first[index, :, columns]
                return
            values = scale * (
                jnp.dot(
                    packed[:, :depth], wv[:depth, columns], preferred_element_type=f32
                )
                + jnp.dot(
                    packed[:, depth:], wv[depth:, columns], preferred_element_type=f32
                )
            )
            used = share * values + (1.0 - share) * first[index, :, columns].astype(f32)
            value_cache[rows, columns] = used.astype(bf16)

        def score(columns, queries, keys):
            halves = (slice(0, head_dim), slice(head_dim, pair))
            normed = [
                [(t[:, h] * inverse_norm(t[:, h])).astype(bf16) for h in halves]
                for t in (queries, keys)
            ]
            key_cache[rows, columns] = jnp.concatenate(normed[1], axis=1)
            low, high = normed[0]
            left = jnp.concatenate(
                [
                    jnp.concatenate([low, blank], axis=1),
                    jnp.concatenate([blank, high], axis=1),
                ],
                axis=0,
            )
            scores = score_scale * lax.dot_general(
                left,
                key_cache[:, columns],
                (((1,), (1,)), ((), ())),
                preferred_element_type=f32,
            )
            weights = jnp.where(causal, jnp.exp(scores), 0.0)
            return weights.astype(bf16), 1.0 / jnp.sum(weights, axis=-1, keepdims=True)

        def attend(columns, weights, inverse):
            both = (
                jnp.dot(weights, value_cache[:, columns], preferred_element_type=f32)
                * inverse
            ).astype(bf16)
            return jnp.concatenate(
                [both[:ROWS, :head_dim], both[ROWS:, head_dim:]], axis=1
            )

        def expand(columns, attended):
            return jnp.dot(attended, wo[columns, :], preferred_element_type=f32)

        c0, c1, c2 = [slice(n * pair, (n + 1) * pair) for n in range(HEADS // 2)]
        p0 = queries_keys(c0)
        p1 = queries_keys(c1)
        p2 = queries_keys(c2)
        s0 = score(c0, *p0)
        used_values(c0)
        s1 = score(c1, *p1)
        used_values(c1)
        s2 = score(c2, *p2)
        used_values(c2)
        a0 = attend(c0, *s0)
        a1 = attend(c1, *s1)
        a2 = attend(c2, *s2)
        e = expand(slice(0, 3 * pair), jnp.concatenate([a0, a1, a2], axis=1))
        following = (hidden + e).astype(bf16)
        leaving[index] = following
        return following

    @pl.when(me == 0)
    def _():
        weight_copies[0].wait()
        make_first(0)
        for n in range(DIRECT):
            first_direct(n).start()
        for copy in weight_copies[1:]:
            copy.wait()

        @pl.loop(0, pieces)
        def _(index):
            layer(index, True)
            hidden_copy(index).start()

            @pl.when(jnp.logical_and(index % 2 == 0, index // 2 + 1 < micro))
            def _():
                make_first(index // 2 + 1)

    @pl.when(me > 0)
    def _():
        for copy in weight_copies:
            copy.wait()

        @pl.when(passes_on)
        def _():
            @pl.loop(0, lead)
            def _(index):
                pass_on(index)

        @pl.loop(0, pieces)
        def _(index):
            @pl.when(jnp.logical_and(passes_on, index + lead < pieces))
            def _():
                pass_on(index + lead)

            hidden_copy(index).wait_recv()

            @pl.when(jnp.logical_or(me == 1, me >= half))
            def _():
                first_along_y(index).wait_recv()

            @pl.when(me == 1)
            def _():
                first_along_z(index).start()

            @pl.when(me == half)
            def _():
                first_along_y(index).start()

            following = layer(index, False)

            @pl.when(me < last)
            def _():
                hidden_copy(index).start()

            @pl.when(me == last)
            def _():
                @pl.when(index // cuts < last)
                def _():
                    result_copy(index).start()

                @pl.when(index // cuts == last)
                def _():
                    result[lax.rem(index, cuts)] = following

    @pl.when(me < last)
    def _():
        @pl.loop(0, cuts)
        def _(index):
            result_copy(index).wait_recv()

    out_copies = [
        pltpu.make_async_copy(
            result.at[n], out_hbm.at[0, pl.ds(n * ROWS, ROWS)], out_sem.at[n]
        )
        for n in range(cuts)
    ]
    for copy in out_copies:
        copy.start()

    @pl.loop(0, pieces)
    def _(index):
        @pl.when(jnp.logical_or(me < last, index // cuts < last))
        def _():
            hidden_copy(index).wait_send()

        @pl.when(
            jnp.logical_or(
                jnp.logical_or(me % half == 0, me == half - 1),
                jnp.logical_and(passes_on, index >= DIRECT),
            )
        )
        def _():
            first_along_y(index).wait_send()

        @pl.when(me < half - 1)
        def _():
            first_along_z(index).wait_send()

    @pl.when(me == 0)
    def _():
        for n in range(DIRECT):
            first_direct(n).wait_send()

    for copy in out_copies:
        copy.wait()


def body(inputs, w_query, w_key, w_value, w_out, mixing):
    sections = lax.axis_size("section")
    micro, seq, width = inputs.shape
    inner = w_query.shape[2]
    cuts = seq // ROWS
    pieces = micro * cuts
    anywhere = pl.BlockSpec(memory_space=pl.ANY)
    dma = pltpu.SemaphoreType.DMA
    return pl.pallas_call(
        functools.partial(kernel, sections),
        out_shape=jax.ShapeDtypeStruct((micro // sections, seq, width), jnp.bfloat16),
        in_specs=[anywhere] * 5 + [pl.BlockSpec(memory_space=pltpu.SMEM)],
        out_specs=anywhere,
        scratch_shapes=[
            pltpu.VMEM((width, inner), jnp.bfloat16),
            pltpu.VMEM((width, inner), jnp.bfloat16),
            pltpu.VMEM((width, inner), jnp.bfloat16),
            pltpu.VMEM((inner, width), jnp.bfloat16),
            pltpu.VMEM((pieces, ROWS, width), jnp.bfloat16),
            pltpu.VMEM((pieces, ROWS, width), jnp.bfloat16),
            pltpu.VMEM((pieces, ROWS, inner), jnp.bfloat16),
            pltpu.VMEM((seq, inner), jnp.bfloat16),
            pltpu.VMEM((seq, inner), jnp.bfloat16),
            pltpu.VMEM((cuts, ROWS, width), jnp.bfloat16),
            dma((4,)),
            dma((pieces,)),
            dma((pieces,)),
            dma((pieces,)),
            dma((pieces,)),
            dma((pieces,)),
            dma((DIRECT,)),
            dma((cuts,)),
            dma((cuts,)),
        ],
        compiler_params=pltpu.CompilerParams(
            collective_id=0, has_side_effects=True, vmem_limit_bytes=60 * 2**20
        ),
    )(inputs, w_query, w_key, w_value, w_out, mixing)


def solution(mesh):
    in_specs = (
        P("dp", None, None),
        P("section", None, None),
        P("section", None, None),
        P("section", None, None),
        P("section", None, None),
        P("section"),
    )
    out_specs = P(("dp", "section"), None, None)
    return jax.shard_map(body, mesh=mesh, in_specs=in_specs, out_specs=out_specs, check_vma=False)
```

```python
import functools

import jax
import jax.numpy as jnp
from jax import lax
from jax.experimental import pallas as pl
from jax.experimental.pallas import tpu as pltpu
from jax.sharding import PartitionSpec as P

MESH = pl.DeviceIdType.MESH
HEADS = 6
ROWS = 32
LEAD = {3: 15, 2: 7}
DIRECT = 2

epsilon = 1e-06
score_scale = 0.12


def inverse_norm(tensor):
    return lax.rsqrt(jnp.mean(tensor * tensor, axis=-1, keepdims=True) + epsilon)


def kernel(
    sections,
    x_hbm,
    wq_hbm,
    wk_hbm,
    wv_hbm,
    wo_hbm,
    mix_ref,
    out_ref,
    wq,
    wk,
    wv,
    wo,
    arrived,
    leaving,
    first,
    key_cache,
    value_cache,
    result,
    weight_sem,
    arrive_sem,
    leave_sem,
    first_sem,
    first_y_sem,
    first_z_sem,
    first_direct_sem,
    result_sem,
):
    me = lax.axis_index("section")
    last = sections - 1
    half = sections // 2
    micro, seq, width = x_hbm.shape
    head_dim = wq.shape[1] // HEADS
    cuts = seq // ROWS
    pieces = micro * cuts
    bf16 = jnp.bfloat16

    weight_copies = [
        pltpu.make_async_copy(source.at[0], target, weight_sem.at[n])
        for n, (source, target) in enumerate(
            ((wv_hbm, wv), (wq_hbm, wq), (wk_hbm, wk), (wo_hbm, wo))
        )
    ]

    def input_copy(index):
        rows = pl.ds(pl.multiple_of(lax.rem(index, cuts) * ROWS, ROWS), ROWS)
        return pltpu.make_async_copy(
            x_hbm.at[index // cuts, rows], arrived.at[index], arrive_sem.at[index]
        )

    def hidden_copy(index):
        return pltpu.make_async_remote_copy(
            src_ref=leaving.at[index],
            dst_ref=arrived.at[index],
            send_sem=leave_sem.at[index],
            recv_sem=arrive_sem.at[index],
            device_id={"section": lax.rem(me + 1, sections)},
            device_id_type=MESH,
        )

    def result_copy(index):
        return pltpu.make_async_remote_copy(
            src_ref=leaving.at[index],
            dst_ref=result.at[lax.rem(index, cuts)],
            send_sem=leave_sem.at[index],
            recv_sem=result_sem.at[lax.rem(index, cuts)],
            device_id={"section": index // cuts},
            device_id_type=MESH,
        )

    def first_along_y(index):
        target = jnp.where(me % half == 0, me + half - 1, me - 1)
        return pltpu.make_async_remote_copy(
            src_ref=first.at[index],
            dst_ref=first.at[index],
            send_sem=first_y_sem.at[index],
            recv_sem=first_sem.at[index],
            device_id={"section": target},
            device_id_type=MESH,
        )

    def first_along_z(index):
        return pltpu.make_async_remote_copy(
            src_ref=first.at[index],
            dst_ref=first.at[index],
            send_sem=first_z_sem.at[index],
            recv_sem=first_sem.at[index],
            device_id={"section": lax.rem(me + half, sections)},
            device_id_type=MESH,
        )

    def first_direct(index):
        return pltpu.make_async_remote_copy(
            src_ref=first.at[index],
            dst_ref=first.at[index],
            send_sem=first_direct_sem.at[index],
            recv_sem=first_sem.at[index],
            device_id={"section": 1},
            device_id_type=MESH,
        )

    @pl.when(me == 0)
    def _():
        for n in range(cuts):
            input_copy(n).start()

    for copy in weight_copies:
        copy.start()

    @pl.when(me == 0)
    def _():
        @pl.loop(cuts, pieces)
        def _(index):
            input_copy(index).start()

    barrier = pltpu.get_barrier_semaphore()
    for step in range(1, sections):
        pl.semaphore_signal(
            barrier,
            inc=1,
            device_id={"section": lax.rem(me + step, sections)},
            device_id_type=MESH,
        )
    key_cache[...] = jnp.zeros_like(key_cache)
    value_cache[...] = jnp.zeros_like(value_cache)
    f32 = jnp.float32
    passes_on = jnp.logical_and(me >= 2, me < half)
    lead = jnp.where(me == half - 1, LEAD[3], LEAD[2])
    share = mix_ref[0]

    def pass_on(index):
        first_along_y(index).wait_recv()

        @pl.when(jnp.logical_or(me == half - 1, index >= DIRECT))
        def _():
            first_along_y(index).start()

        @pl.when(me == 2)
        def _():
            first_along_z(index).start()

    def make_first(sequence):
        base = sequence * cuts
        for n in range(cuts):
            input_copy(base + n).wait()
        packed = jnp.concatenate([arrived[base + n] for n in range(cuts)], axis=0)
        scale = inverse_norm(packed.astype(f32))
        values = scale * jnp.dot(packed, wv[...], preferred_element_type=f32)
        for n in range(cuts):
            first[base + n] = values[n * ROWS : (n + 1) * ROWS].astype(bf16)

    def send_first(sequence):
        for n in range(cuts):
            first_along_y(sequence * cuts + n).start()
            first_along_z(sequence * cuts + n).start()

    def layer(index, origin):
        cut = lax.rem(index, cuts)
        start = pl.multiple_of(cut * ROWS, ROWS)
        rows = pl.ds(start, ROWS)
        packed = arrived[index]
        hidden = packed.astype(f32)
        scale = inverse_norm(hidden)
        query_at = start + lax.broadcasted_iota(jnp.int32, (2 * ROWS, seq), 0) % ROWS
        key_at = lax.broadcasted_iota(jnp.int32, (2 * ROWS, seq), 1)
        causal = query_at >= key_at
        blank = jnp.zeros((ROWS, head_dim), bf16)
        pair = 2 * head_dim
        def queries_keys(columns):
            return [
                scale * jnp.dot(packed, w[:, columns], preferred_element_type=f32)
                for w in (wq, wk)
            ]

        def used_values(columns):
            if origin:
                value_cache[rows, columns] = first[index, :, columns]
                return
            values = scale * jnp.dot(packed, wv[:, columns], preferred_element_type=f32)
            used = share * values + (1.0 - share) * first[index, :, columns].astype(f32)
            value_cache[rows, columns] = used.astype(bf16)

        def score(columns, queries, keys):
            halves = (slice(0, head_dim), slice(head_dim, pair))
            normed = [
                [(t[:, h] * inverse_norm(t[:, h])).astype(bf16) for h in halves]
                for t in (queries, keys)
            ]
            key_cache[rows, columns] = jnp.concatenate(normed[1], axis=1)
            low, high = normed[0]
            left = jnp.concatenate(
                [
                    jnp.concatenate([low, blank], axis=1),
                    jnp.concatenate([blank, high], axis=1),
                ],
                axis=0,
            )
            scores = score_scale * lax.dot_general(
                left,
                key_cache[:, columns],
                (((1,), (1,)), ((), ())),
                preferred_element_type=f32,
            )
            weights = jnp.where(causal, jnp.exp(scores), 0.0)
            return weights.astype(bf16), 1.0 / jnp.sum(weights, axis=-1, keepdims=True)

        def attend(columns, weights, inverse):
            both = (
                jnp.dot(weights, value_cache[:, columns], preferred_element_type=f32)
                * inverse
            ).astype(bf16)
            return jnp.concatenate(
                [both[:ROWS, :head_dim], both[ROWS:, head_dim:]], axis=1
            )

        def expand(columns, attended):
            return jnp.dot(attended, wo[columns, :], preferred_element_type=f32)

        c0, c1, c2 = [slice(n * pair, (n + 1) * pair) for n in range(HEADS // 2)]
        p0 = queries_keys(c0)
        p1 = queries_keys(c1)
        p2 = queries_keys(c2)
        used_values(slice(0, 3 * pair))
        s0 = score(c0, *p0)
        s1 = score(c1, *p1)
        s2 = score(c2, *p2)
        a0 = attend(c0, *s0)
        a1 = attend(c1, *s1)
        a2 = attend(c2, *s2)
        e = expand(slice(0, 3 * pair), jnp.concatenate([a0, a1, a2], axis=1))
        following = (hidden + e).astype(bf16)
        leaving[index] = following
        return following

    @pl.when(me == 0)
    def _():
        weight_copies[0].wait()
        make_first(0)

    pl.semaphore_wait(barrier, sections - 1)

    @pl.when(me == 0)
    def _():
        send_first(0)
        for n in range(DIRECT):
            first_direct(n).start()
        for copy in weight_copies[1:]:
            copy.wait()

        @pl.loop(0, pieces)
        def _(index):
            layer(index, True)
            hidden_copy(index).start()

            @pl.when(jnp.logical_and(index % 2 == 0, index // 2 + 1 < micro))
            def _():
                make_first(index // 2 + 1)
                send_first(index // 2 + 1)

    @pl.when(me > 0)
    def _():
        for copy in weight_copies:
            copy.wait()

        @pl.when(passes_on)
        def _():
            @pl.loop(0, lead)
            def _(index):
                pass_on(index)

        @pl.loop(0, pieces)
        def _(index):
            @pl.when(jnp.logical_and(passes_on, index + lead < pieces))
            def _():
                pass_on(index + lead)

            hidden_copy(index).wait_recv()

            @pl.when(jnp.logical_or(me == 1, me >= half))
            def _():
                first_along_y(index).wait_recv()

            @pl.when(me == 1)
            def _():
                first_along_z(index).start()

            @pl.when(me == half)
            def _():
                first_along_y(index).start()

            following = layer(index, False)

            @pl.when(me < last)
            def _():
                hidden_copy(index).start()

            @pl.when(me == last)
            def _():
                @pl.when(index // cuts < last)
                def _():
                    result_copy(index).start()

                @pl.when(index // cuts == last)
                def _():
                    result[lax.rem(index, cuts)] = following

    @pl.when(me < last)
    def _():
        @pl.loop(0, cuts)
        def _(index):
            result_copy(index).wait_recv()

    for n in range(cuts):
        out_ref[0, n * ROWS : (n + 1) * ROWS] = result[n]

    @pl.loop(0, pieces)
    def _(index):
        @pl.when(jnp.logical_or(me < last, index // cuts < last))
        def _():
            hidden_copy(index).wait_send()

        @pl.when(
            jnp.logical_or(
                jnp.logical_or(me % half == 0, me == half - 1),
                jnp.logical_and(passes_on, index >= DIRECT),
            )
        )
        def _():
            first_along_y(index).wait_send()

        @pl.when(me < half - 1)
        def _():
            first_along_z(index).wait_send()

    @pl.when(me == 0)
    def _():
        for n in range(DIRECT):
            first_direct(n).wait_send()


def body(inputs, w_query, w_key, w_value, w_out, mixing):
    sections = lax.axis_size("section")
    micro, seq, width = inputs.shape
    inner = w_query.shape[2]
    cuts = seq // ROWS
    pieces = micro * cuts
    anywhere = pl.BlockSpec(memory_space=pl.ANY)
    dma = pltpu.SemaphoreType.DMA
    return pl.pallas_call(
        functools.partial(kernel, sections),
        out_shape=jax.ShapeDtypeStruct((micro // sections, seq, width), jnp.bfloat16),
        in_specs=[anywhere] * 5 + [pl.BlockSpec(memory_space=pltpu.SMEM)],
        out_specs=pl.BlockSpec(memory_space=pltpu.VMEM),
        scratch_shapes=[
            pltpu.VMEM((width, inner), jnp.bfloat16),
            pltpu.VMEM((width, inner), jnp.bfloat16),
            pltpu.VMEM((width, inner), jnp.bfloat16),
            pltpu.VMEM((inner, width), jnp.bfloat16),
            pltpu.VMEM((pieces, ROWS, width), jnp.bfloat16),
            pltpu.VMEM((pieces, ROWS, width), jnp.bfloat16),
            pltpu.VMEM((pieces, ROWS, inner), jnp.bfloat16),
            pltpu.VMEM((seq, inner), jnp.bfloat16),
            pltpu.VMEM((seq, inner), jnp.bfloat16),
            pltpu.VMEM((cuts, ROWS, width), jnp.bfloat16),
            dma((4,)),
            dma((pieces,)),
            dma((pieces,)),
            dma((pieces,)),
            dma((pieces,)),
            dma((pieces,)),
            dma((DIRECT,)),
            dma((cuts,)),
        ],
        compiler_params=pltpu.CompilerParams(
            collective_id=0, has_side_effects=True, vmem_limit_bytes=53 * 2**20
        ),
    )(inputs, w_query, w_key, w_value, w_out, mixing)


def solution(mesh):
    in_specs = (
        P("dp", None, None),
        P("section", None, None),
        P("section", None, None),
        P("section", None, None),
        P("section", None, None),
        P("section"),
    )
    out_specs = P(("dp", "section"), None, None)
    return jax.shard_map(body, mesh=mesh, in_specs=in_specs, out_specs=out_specs, check_vma=False)
```

```python
import functools

import jax
import jax.numpy as jnp
from jax import lax
from jax.experimental import pallas as pl
from jax.experimental.pallas import tpu as pltpu
from jax.sharding import PartitionSpec as P

MESH = pl.DeviceIdType.MESH
HEADS = 6
ROWS = 32
LEAD = {3: 15, 2: 7}
DIRECT = 2

epsilon = 1e-06
score_scale = 0.12


def inverse_norm(tensor):
    return lax.rsqrt(jnp.mean(tensor * tensor, axis=-1, keepdims=True) + epsilon)


def kernel(
    sections,
    x_hbm,
    wq_hbm,
    wk_hbm,
    wv_hbm,
    wo_hbm,
    mix_ref,
    out_ref,
    wq,
    wk,
    wv,
    wo,
    arrived,
    leaving,
    first,
    key_cache,
    value_cache,
    result,
    weight_sem,
    arrive_sem,
    leave_sem,
    first_sem,
    first_y_sem,
    first_z_sem,
    first_direct_sem,
    result_sem,
):
    me = lax.axis_index("section")
    last = sections - 1
    half = sections // 2
    micro, seq, width = x_hbm.shape
    head_dim = wq.shape[1] // HEADS
    cuts = seq // ROWS
    pieces = micro * cuts
    bf16 = jnp.bfloat16

    weight_copies = [
        pltpu.make_async_copy(source.at[0], target, weight_sem.at[n])
        for n, (source, target) in enumerate(
            ((wv_hbm, wv), (wq_hbm, wq), (wk_hbm, wk), (wo_hbm, wo))
        )
    ]

    def input_copy(index):
        rows = pl.ds(pl.multiple_of(lax.rem(index, cuts) * ROWS, ROWS), ROWS)
        return pltpu.make_async_copy(
            x_hbm.at[index // cuts, rows], arrived.at[index], arrive_sem.at[index]
        )

    def hidden_copy(index):
        return pltpu.make_async_remote_copy(
            src_ref=leaving.at[index],
            dst_ref=arrived.at[index],
            send_sem=leave_sem.at[index],
            recv_sem=arrive_sem.at[index],
            device_id={"section": lax.rem(me + 1, sections)},
            device_id_type=MESH,
        )

    def result_copy(index):
        return pltpu.make_async_remote_copy(
            src_ref=leaving.at[index],
            dst_ref=result.at[lax.rem(index, cuts)],
            send_sem=leave_sem.at[index],
            recv_sem=result_sem.at[lax.rem(index, cuts)],
            device_id={"section": index // cuts},
            device_id_type=MESH,
        )

    def first_along_y(index):
        target = jnp.where(me % half == 0, me + half - 1, me - 1)
        return pltpu.make_async_remote_copy(
            src_ref=first.at[index],
            dst_ref=first.at[index],
            send_sem=first_y_sem.at[index],
            recv_sem=first_sem.at[index],
            device_id={"section": target},
            device_id_type=MESH,
        )

    def first_along_z(index):
        return pltpu.make_async_remote_copy(
            src_ref=first.at[index],
            dst_ref=first.at[index],
            send_sem=first_z_sem.at[index],
            recv_sem=first_sem.at[index],
            device_id={"section": lax.rem(me + half, sections)},
            device_id_type=MESH,
        )

    def first_direct(index):
        return pltpu.make_async_remote_copy(
            src_ref=first.at[index],
            dst_ref=first.at[index],
            send_sem=first_direct_sem.at[index],
            recv_sem=first_sem.at[index],
            device_id={"section": 1},
            device_id_type=MESH,
        )

    @pl.when(me == 0)
    def _():
        for n in range(cuts):
            input_copy(n).start()

    for copy in weight_copies:
        copy.start()

    @pl.when(me == 0)
    def _():
        @pl.loop(cuts, pieces)
        def _(index):
            input_copy(index).start()

    barrier = pltpu.get_barrier_semaphore()
    for step in range(1, sections):
        pl.semaphore_signal(
            barrier,
            inc=1,
            device_id={"section": lax.rem(me + step, sections)},
            device_id_type=MESH,
        )
    key_cache[...] = jnp.zeros_like(key_cache)
    value_cache[...] = jnp.zeros_like(value_cache)
    f32 = jnp.float32
    passes_on = jnp.logical_and(me >= 2, me < half)
    lead = jnp.where(me == half - 1, LEAD[3], LEAD[2])
    share = mix_ref[0]

    def pass_on(index):
        first_along_y(index).wait_recv()

        @pl.when(jnp.logical_or(me == half - 1, index >= DIRECT))
        def _():
            first_along_y(index).start()

        @pl.when(me == 2)
        def _():
            first_along_z(index).start()

    def make_first(sequence):
        base = sequence * cuts
        for n in range(cuts):
            input_copy(base + n).wait()
        packed = jnp.concatenate([arrived[base + n] for n in range(cuts)], axis=0)
        scale = inverse_norm(packed.astype(f32))
        values = scale * jnp.dot(packed, wv[...], preferred_element_type=f32)
        for n in range(cuts):
            first[base + n] = values[n * ROWS : (n + 1) * ROWS].astype(bf16)

    def send_first(sequence):
        for n in range(cuts):
            first_along_y(sequence * cuts + n).start()
            first_along_z(sequence * cuts + n).start()

    def layer(index, origin):
        cut = lax.rem(index, cuts)
        start = pl.multiple_of(cut * ROWS, ROWS)
        rows = pl.ds(start, ROWS)
        packed = arrived[index]
        hidden = packed.astype(f32)
        scale = inverse_norm(hidden)
        query_at = start + lax.broadcasted_iota(jnp.int32, (2 * ROWS, seq), 0) % ROWS
        key_at = lax.broadcasted_iota(jnp.int32, (2 * ROWS, seq), 1)
        causal = query_at >= key_at
        blank = jnp.zeros((ROWS, head_dim), bf16)
        pair = 2 * head_dim
        def queries_keys(columns):
            return [
                scale * jnp.dot(packed, w[:, columns], preferred_element_type=f32)
                for w in (wq, wk)
            ]

        def used_values(columns):
            if origin:
                value_cache[rows, columns] = first[index, :, columns]
                return
            values = scale * jnp.dot(packed, wv[:, columns], preferred_element_type=f32)
            used = share * values + (1.0 - share) * first[index, :, columns].astype(f32)
            value_cache[rows, columns] = used.astype(bf16)

        def score(columns, queries, keys):
            halves = (slice(0, head_dim), slice(head_dim, pair))
            normed = [
                [(t[:, h] * inverse_norm(t[:, h])).astype(bf16) for h in halves]
                for t in (queries, keys)
            ]
            key_cache[rows, columns] = jnp.concatenate(normed[1], axis=1)
            low, high = normed[0]
            left = jnp.concatenate(
                [
                    jnp.concatenate([low, blank], axis=1),
                    jnp.concatenate([blank, high], axis=1),
                ],
                axis=0,
            )
            scores = score_scale * lax.dot_general(
                left,
                key_cache[:, columns],
                (((1,), (1,)), ((), ())),
                preferred_element_type=f32,
            )
            weights = jnp.where(causal, jnp.exp(scores), 0.0)
            return weights.astype(bf16), 1.0 / jnp.sum(weights, axis=-1, keepdims=True)

        def attend(columns, weights, inverse):
            both = (
                jnp.dot(weights, value_cache[:, columns], preferred_element_type=f32)
                * inverse
            ).astype(bf16)
            return jnp.concatenate(
                [both[:ROWS, :head_dim], both[ROWS:, head_dim:]], axis=1
            )

        def expand(columns, attended):
            return jnp.dot(attended, wo[columns, :], preferred_element_type=f32)

        c0, c1, c2 = [slice(n * pair, (n + 1) * pair) for n in range(HEADS // 2)]
        p0 = queries_keys(c0)
        p1 = queries_keys(c1)
        p2 = queries_keys(c2)
        used_values(slice(0, 3 * pair))
        s0 = score(c0, *p0)
        s1 = score(c1, *p1)
        s2 = score(c2, *p2)
        a0 = attend(c0, *s0)
        a1 = attend(c1, *s1)
        a2 = attend(c2, *s2)
        e = expand(slice(0, 3 * pair), jnp.concatenate([a0, a1, a2], axis=1))
        following = (hidden + e).astype(bf16)
        leaving[index] = following
        return following

    @pl.when(me == 0)
    def _():
        weight_copies[0].wait()
        make_first(0)

    pl.semaphore_wait(barrier, sections - 1)

    @pl.when(me == 0)
    def _():
        send_first(0)
        for n in range(DIRECT):
            first_direct(n).start()
        for copy in weight_copies[1:]:
            copy.wait()

        @pl.loop(0, pieces)
        def _(index):
            layer(index, True)
            hidden_copy(index).start()

            @pl.when(jnp.logical_and(index % 2 == 0, index // 2 + 1 < micro))
            def _():
                make_first(index // 2 + 1)
                send_first(index // 2 + 1)

    @pl.when(me > 0)
    def _():
        for copy in weight_copies:
            copy.wait()

        @pl.when(passes_on)
        def _():
            @pl.loop(0, lead)
            def _(index):
                pass_on(index)

        @pl.loop(0, pieces)
        def _(index):
            @pl.when(jnp.logical_and(passes_on, index + lead < pieces))
            def _():
                pass_on(index + lead)

            hidden_copy(index).wait_recv()

            @pl.when(jnp.logical_or(me == 1, me >= half))
            def _():
                first_along_y(index).wait_recv()

            @pl.when(me == 1)
            def _():
                first_along_z(index).start()

            @pl.when(me == half)
            def _():
                first_along_y(index).start()

            following = layer(index, False)

            @pl.when(me < last)
            def _():
                hidden_copy(index).start()

            @pl.when(me == last)
            def _():
                @pl.when(index >= cuts)
                def _():
                    result_copy(index - cuts).wait_send()

                @pl.when(index // cuts < last)
                def _():
                    result_copy(index).start()

                @pl.when(index // cuts == last)
                def _():
                    result[lax.rem(index, cuts)] = following

    @pl.when(me < last)
    def _():
        @pl.loop(0, cuts)
        def _(index):
            result_copy(index).wait_recv()

    for n in range(cuts):
        out_ref[0, n * ROWS : (n + 1) * ROWS] = result[n]

    @pl.when(me < last)
    def _():
        @pl.loop(0, pieces)
        def _(index):
            hidden_copy(index).wait_send()

            @pl.when(
                jnp.logical_or(
                    jnp.logical_or(me % half == 0, me == half - 1),
                    jnp.logical_and(passes_on, index >= DIRECT),
                )
            )
            def _():
                first_along_y(index).wait_send()

            @pl.when(me < half - 1)
            def _():
                first_along_z(index).wait_send()

    @pl.when(me == 0)
    def _():
        for n in range(DIRECT):
            first_direct(n).wait_send()


def body(inputs, w_query, w_key, w_value, w_out, mixing):
    sections = lax.axis_size("section")
    micro, seq, width = inputs.shape
    inner = w_query.shape[2]
    cuts = seq // ROWS
    pieces = micro * cuts
    anywhere = pl.BlockSpec(memory_space=pl.ANY)
    dma = pltpu.SemaphoreType.DMA
    return pl.pallas_call(
        functools.partial(kernel, sections),
        out_shape=jax.ShapeDtypeStruct((micro // sections, seq, width), jnp.bfloat16),
        in_specs=[anywhere] * 5 + [pl.BlockSpec(memory_space=pltpu.SMEM)],
        out_specs=pl.BlockSpec(memory_space=pltpu.VMEM),
        scratch_shapes=[
            pltpu.VMEM((width, inner), jnp.bfloat16),
            pltpu.VMEM((width, inner), jnp.bfloat16),
            pltpu.VMEM((width, inner), jnp.bfloat16),
            pltpu.VMEM((inner, width), jnp.bfloat16),
            pltpu.VMEM((pieces, ROWS, width), jnp.bfloat16),
            pltpu.VMEM((pieces, ROWS, width), jnp.bfloat16),
            pltpu.VMEM((pieces, ROWS, inner), jnp.bfloat16),
            pltpu.VMEM((seq, inner), jnp.bfloat16),
            pltpu.VMEM((seq, inner), jnp.bfloat16),
            pltpu.VMEM((cuts, ROWS, width), jnp.bfloat16),
            dma((4,)),
            dma((pieces,)),
            dma((pieces,)),
            dma((pieces,)),
            dma((pieces,)),
            dma((pieces,)),
            dma((DIRECT,)),
            dma((cuts,)),
        ],
        compiler_params=pltpu.CompilerParams(
            collective_id=0, has_side_effects=True, vmem_limit_bytes=53 * 2**20
        ),
    )(inputs, w_query, w_key, w_value, w_out, mixing)


def solution(mesh):
    in_specs = (
        P("dp", None, None),
        P("section", None, None),
        P("section", None, None),
        P("section", None, None),
        P("section", None, None),
        P("section"),
    )
    out_specs = P(("dp", "section"), None, None)
    return jax.shard_map(body, mesh=mesh, in_specs=in_specs, out_specs=out_specs, check_vma=False)
```
